32 devices in a mesh: grp: 4 (over z), loc: 8 (over y, x, core).
Axes of the slice: x: 2, y: 2, z: 4, core: 2. Of those that a mesh axis runs over, the one named last changes fastest.
Arguments:
- features: float32 [32768, 256], P(('grp', 'loc')), may hold values from -6 to 6
- hub_block: bfloat16 [128, 32768], P(None, ('grp', 'loc')), may hold values from -0.0625 to 0.0625
- hub_slot: int32 [128], P(('grp', 'loc')), may hold values from 0 to 1023, as said below
- neighbours: int32 [32768, 16], P(('grp', 'loc')), may hold values from 0 to 2047
- counts: int32 [32768], P(('grp', 'loc')), may hold values from 1 to 16
- halo_send: int32 [256, 128], P(('grp', 'loc')), may hold values from 0 to 1023
- weight: float32 [256, 256], replicated, may hold values from -0.375 to 0.375
- bias: float32 [256], replicated, may hold values from -3 to 3
Outputs:
- layer_out: float32 [32768, 256], P(('grp', 'loc'))
The draws below stay inside these ranges and needn't reach their ends.
Inputs may be any that keep to these rules, and one draw needn't show every extreme that they name: `hub_slot`: within each aligned block of 4 entries the values are distinct.
All inputs are finite; a program needn't handle non-finite values.
Results may differ from the reference program's by a relative error of at most 0.0003.
Values sent between devices are 32-bit elements; how exact they have to be, the bound alone decides.
No kernel may reach another device: no remote copies, remote signals or barrier semaphores. Data moves between devices by JAX's collectives and lax.ppermute only.
A program may use at most 64 MiB of HBM per device.

```python
import jax
import jax.numpy as jnp
from jax import lax

F = 256
V_DEV = 1024
HUB_DEV = 4
K = 16
S = 128
V = 32768
HUB = 128
N_GRP = 4
N_LOC = 8
DEVICES = 32


def draw_hub_slot(key, part):
    owners = HUB // HUB_DEV
    keys = jax.random.split(jax.random.fold_in(key, 11), owners)
    picked = jax.vmap(lambda single: jax.random.permutation(single, V_DEV)[:HUB_DEV])(keys)
    return picked.reshape(-1).astype(jnp.int32)


def place_ends(array, stream_key, least, largest):
    shape = array.shape
    spot = [jax.random.randint(jax.random.fold_in(stream_key, axis), (), 0, shape[axis]) for axis in range(len(shape))]
    array = array.at[tuple(spot)].set(least)
    longest = shape.index(max(shape))
    spot[longest] = (spot[longest] + 1) % shape[longest]
    return array.at[tuple(spot)].set(largest)


def spiked(entries, own_key, source, target, blocks, factor):
    def block_of(position):
        return (jnp.arange(entries.shape[position]) // (entries.shape[position] // blocks)).reshape((-1,) + (1,) * (entries.ndim - 1 - position))

    first = jax.random.permutation(own_key, blocks)[block_of(target)]
    other_side = (block_of(target) + blocks // 2) % blocks
    return jnp.where((block_of(source) == first) | (block_of(source) == other_side), factor * entries, entries)


def block_levels(key, extent, cuts, low, top_value):
    def one(dim, shards_of):
        draws = jax.random.uniform(jax.random.fold_in(jax.random.fold_in(key, 6), dim), (shards_of,), jnp.float32, low / len(cuts), top_value / len(cuts))
        return jnp.repeat(jnp.exp(draws), extent[dim] // shards_of).reshape((-1,) + (1,) * (len(extent) - dim - 1))

    loudness = one(*cuts[0])
    for cut in cuts[1:]:
        loudness = loudness * one(*cut)
    return loudness


def centred(key, extent, width, bound, cuts=(), kind=jnp.bfloat16):
    array = jax.random.normal(key, extent, jnp.float32) * width
    if len(cuts) > 0:
        array = block_levels(key, extent, cuts, -0.22, 0.18) * array
    return jnp.clip(array, min=-bound, max=bound).astype(kind)


def heavy_noise(key, extent, deviation, most, cuts, heavy, kind=jnp.bfloat16):
    entries = deviation * jax.random.normal(key, extent, jnp.float32)
    if cuts:
        entries = entries * block_levels(key, extent, cuts, -0.22, 0.18)
    return jnp.clip(spiked(entries, jax.random.fold_in(key, 3), *heavy), -most, most).astype(kind)


def setup_inputs(seed: int = 0) -> dict:
    splits = jax.random.split(jax.random.key(seed), 9)
    return {
        "features": centred(splits[0], (V, F), 1.0, 6.0, ((0, 32),), jnp.float32),
        "hub_block": heavy_noise(splits[1], (HUB, V), V ** -0.5, 0.0625, ((1, 32),), (1, 0, 32, 2.75)),
        "hub_slot": draw_hub_slot(jax.random.fold_in(splits[8], 71), 0),
        "neighbours": place_ends(jax.random.randint(splits[3], (V, K), 0, V_DEV + N_LOC * S), jax.random.fold_in(splits[3], 1), 0, (V_DEV + N_LOC * S) - 1).astype(jnp.int32),
        "counts": place_ends(jax.random.randint(splits[4], (V,), 1, K + 1), jax.random.fold_in(splits[4], 1), 1, K).astype(jnp.int32),
        "halo_send": place_ends(jax.random.randint(splits[5], (DEVICES * N_LOC, S), 0, V_DEV), jax.random.fold_in(splits[5], 1), 0, V_DEV - 1).astype(jnp.int32),
        "weight": centred(splits[6], (F, F), F ** -0.5, 0.375, (), jnp.float32),
        "bias": centred(splits[7], (F,), 0.5, 3.0, (), jnp.float32),
    }


def reference(features, hub_block, hub_slot, neighbours, counts, halo_send, weight, bias):
    rounded = features.astype(jnp.bfloat16)
    hub_sum = jnp.dot(hub_block, rounded, preferred_element_type=jnp.float32)
    devices = N_GRP * N_LOC
    send_table = halo_send.reshape(devices, N_LOC, S)
    nbr_blocks = neighbours.reshape(devices, V_DEV, K)
    cnt_blocks = counts.reshape(devices, V_DEV)

    def one_device(device):
        group = device // N_LOC
        place = device % N_LOC
        peers = (group * N_LOC + jnp.arange(N_LOC)).astype(jnp.int32)
        sent_rows = send_table[peers, place]
        remote_ids = (peers[:, None] * V_DEV + sent_rows).reshape(-1)
        own_ids = (device * V_DEV + jnp.arange(V_DEV)).astype(jnp.int32)
        ids_table = jnp.concatenate([own_ids, remote_ids.astype(jnp.int32)])
        slots = nbr_blocks[device]
        gathered = features[ids_table[slots]]
        used = (jnp.arange(K)[None, :] < cnt_blocks[device][:, None]).astype(jnp.float32)
        summed = jnp.sum(gathered * used[:, :, None], axis=1)
        return summed / cnt_blocks[device].astype(jnp.float32)[:, None]

    low = lax.map(one_device, jnp.arange(devices).astype(jnp.int32)).reshape(-1, F)
    combined = features + low
    targets = (jnp.arange(HUB) // HUB_DEV).astype(jnp.int32) * V_DEV + hub_slot
    combined = combined.at[targets].add(hub_sum)
    result = jnp.dot(combined, weight, precision=lax.Precision.HIGHEST, preferred_element_type=jnp.float32) + bias
    return jnp.maximum(result, 0.0)
```

```python
import functools

import jax
import jax.numpy as jnp
from jax import lax
from jax.experimental import pallas as pl
from jax.experimental.pallas import tpu as pltpu
from jax.sharding import PartitionSpec as P

BF = jnp.bfloat16
F32 = jnp.float32
LANES = 128
GROUP = 16


def split(x):
    hi = x.astype(BF)
    return hi, (x - hi.astype(F32)).astype(BF)


def mm(a, b, dims=((1,), (0,))):
    return lax.dot_general(a, b, (dims, ((), ())), preferred_element_type=F32)


def pick_kernel(features, halo, out, *, peers, rows):
    hi, lo = split(features[...])
    own = features.shape[0]
    listed = halo[...].T
    col = lax.broadcasted_iota(jnp.int32, (rows, own), 1)
    for q in range(peers):
        hot = (listed[:, q : q + 1] == col).astype(F32).astype(BF)
        out[q] = mm(hot, hi) + mm(hot, lo)


def hub_kernel(me, features, hub, *refs, parts):
    outs, full = refs[:parts], refs[parts]
    full[...] = mm(hub[...], features[...].astype(BF))
    size = full.shape[0] // parts
    for s in range(parts):
        at = pl.multiple_of((me[0] ^ s) * size, size)
        outs[s][...] = full[pl.ds(at, size), :]


def inverse_counts(counts):
    return 1.0 / counts[...].astype(F32).T


def count_kernel(features, slots, counts, adj, base, local, *, degree, pool):
    own, width = features.shape
    span = GROUP * degree
    near = own // LANES
    codes = pool // LANES
    row = lax.broadcasted_iota(jnp.int32, (codes * GROUP, span), 0)
    lane = lax.broadcasted_iota(jnp.int32, (LANES, span), 0)
    vert = lax.broadcasted_iota(jnp.int32, (1, span), 1) // degree

    def build(b, _):
        name = slots[pl.ds(b, 1), :]
        code = jnp.where(name < 0, -1, (name // LANES) * GROUP + vert)
        left = (row == code).astype(F32).astype(BF)
        right = (lane == (name & (LANES - 1))).astype(F32).astype(BF)
        made = mm(left, right, ((1,), (1,))).astype(BF)
        at = pl.multiple_of(b * GROUP, GROUP)
        for h in range(codes):
            part = made[h * GROUP : (h + 1) * GROUP]
            if h < near:
                local[pl.ds(at, GROUP), h * LANES : (h + 1) * LANES] = part
            else:
                adj[pl.ds(at, GROUP), (h - near) * LANES : (h - near + 1) * LANES] = part
        return 0

    lax.fori_loop(0, own // GROUP, build, 0, unroll=4)
    hi, lo = split(features[...])
    inv = inverse_counts(counts)
    for j in range(own // LANES):
        cut = slice(j * LANES, (j + 1) * LANES)
        a = local[cut, :]
        base[cut, :] = features[cut, :] + (mm(a, hi) + mm(a, lo)) * inv[:, j : j + 1]


def last_kernel(slot, adj, received, base, counts, hub, weight, bias, out, comb):
    own, width = base.shape
    hi, lo = split(received[...])
    inv = inverse_counts(counts)
    for j in range(own // LANES):
        cut = slice(j * LANES, (j + 1) * LANES)
        a = adj[cut, :]
        comb[cut, :] = base[cut, :] + (mm(a, hi) + mm(a, lo)) * inv[:, j : j + 1]
    sums = jnp.sum(hub[...], axis=0)
    for i in range(sums.shape[0]):
        at = slot[i]
        comb[pl.ds(at, 1), :] = comb[pl.ds(at, 1), :] + sums[i : i + 1]
    whi, wlo = split(weight[...])
    for j in range(own // LANES):
        cut = slice(j * LANES, (j + 1) * LANES)
        chi, clo = split(comb[cut, :])
        made = mm(chi, whi) + (mm(chi, wlo) + mm(clo, whi)) + bias[...]
        out[cut, :] = jnp.maximum(made, 0.0)


VMEM = pl.BlockSpec(memory_space=pltpu.VMEM)
SMEM = pl.BlockSpec(memory_space=pltpu.SMEM)
PARAMS = pltpu.CompilerParams(vmem_limit_bytes=24 * 1024 * 1024)


def flops(n):
    return pl.CostEstimate(flops=n, bytes_accessed=1 << 20, transcendentals=0)


def on_device(features, hub_block, hub_slot, neighbours, counts, halo_send, weight, bias):
    own, width = features.shape
    degree = neighbours.shape[1]
    n_grp, n_loc = lax.axis_size("grp"), lax.axis_size("loc")
    listed = halo_send.shape[1]
    hubs = hub_block.shape[0]
    owned = hub_slot.shape[0]
    pool = own + n_loc * listed
    me = lax.axis_index("grp").astype(jnp.int32).reshape(1)

    outgoing = pl.pallas_call(
        functools.partial(pick_kernel, peers=n_loc, rows=listed),
        out_shape=jax.ShapeDtypeStruct((n_loc, listed, width), F32),
        in_specs=[VMEM] * 2,
        out_specs=VMEM,
        compiler_params=PARAMS,
        cost_estimate=flops(4 * n_loc * listed * own * width),
        name="pick",
    )(features, halo_send)
    received = lax.all_to_all(outgoing, "loc", split_axis=0, concat_axis=0, tiled=True)

    part_rows = hubs // n_grp
    parts = pl.pallas_call(
        functools.partial(hub_kernel, parts=n_grp),
        out_shape=[jax.ShapeDtypeStruct((part_rows, width), F32)] * n_grp,
        in_specs=[SMEM, VMEM, VMEM],
        out_specs=[VMEM] * n_grp,
        scratch_shapes=[pltpu.VMEM((hubs, width), F32)],
        compiler_params=PARAMS,
        cost_estimate=flops(2 * hubs * own * width),
        name="hub",
    )(me, features, hub_block)
    group_part = parts[0]
    for s in range(1, n_grp):
        pairs = [(i, i ^ s) for i in range(n_grp)]
        group_part = group_part + lax.ppermute(parts[s], "grp", pairs)
    group_part = group_part.reshape(n_loc, owned, width)
    hub_pieces = lax.all_to_all(group_part, "loc", split_axis=0, concat_axis=0, tiled=True)

    used = jnp.arange(degree, dtype=jnp.int32)[None, :] < counts[:, None]
    slots = jnp.where(used, neighbours, -1).reshape(own // GROUP, GROUP * degree)
    counts_rows = counts.reshape(own // LANES, LANES)
    adj, base = pl.pallas_call(
        functools.partial(count_kernel, degree=degree, pool=pool),
        out_shape=[
            jax.ShapeDtypeStruct((own, pool - own), BF),
            jax.ShapeDtypeStruct((own, width), F32),
        ],
        in_specs=[VMEM] * 3,
        out_specs=[VMEM] * 2,
        scratch_shapes=[pltpu.VMEM((own, own), BF)],
        compiler_params=PARAMS,
        cost_estimate=flops(8 * own * own * width),
        name="count",
    )(features, slots, counts_rows)

    return pl.pallas_call(
        last_kernel,
        out_shape=jax.ShapeDtypeStruct((own, width), F32),
        in_specs=[SMEM] + [VMEM] * 7,
        out_specs=VMEM,
        scratch_shapes=[pltpu.VMEM((own, width), F32)],
        compiler_params=PARAMS,
        cost_estimate=flops(8 * own * own * width),
        name="last",
    )(
        hub_slot,
        adj,
        received.reshape(n_loc * listed, width),
        base,
        counts_rows,
        hub_pieces,
        weight,
        bias.reshape(1, width),
    )


def solution(mesh):
    in_specs = (
        P(("grp", "loc"), None),
        P(None, ("grp", "loc")),
        P(("grp", "loc")),
        P(("grp", "loc"), None),
        P(("grp", "loc")),
        P(("grp", "loc"), None),
        P(),
        P(),
    )
    out_specs = P(("grp", "loc"), None)
    return jax.shard_map(
        on_device, mesh=mesh, in_specs=in_specs, out_specs=out_specs, check_vma=False
    )
```

```python
import functools

import jax
import jax.numpy as jnp
from jax import lax
from jax.experimental import pallas as pl
from jax.experimental.pallas import tpu as pltpu
from jax.sharding import PartitionSpec as P


BF = jnp.bfloat16
F32 = jnp.float32
LANES = 128
STEPS = 4
GROUP = 16


def FLOW(peers):
    return sorted(range(1, peers), key=lambda s: (s < 2, s & 1, -s)) + [0]


def split(x):
    hi = x.astype(BF)
    return hi, (x - hi.astype(F32)).astype(BF)


def mm(a, b, dims=((1,), (0,))):
    return lax.dot_general(a, b, (dims, ((), ())), preferred_element_type=F32)


def pick_kernel(me, features, halo, *refs, peers, rows):
    outs, order = refs[:peers], refs[peers]
    hi, lo = split(features[...])
    own = features.shape[0]
    for s in range(peers):
        order[s : s + 1, :] = halo[pl.ds(me[1] ^ s, 1), :]
    listed = order[...].T
    col = lax.broadcasted_iota(jnp.int32, (rows, own), 1)
    for s in FLOW(peers):
        hot = (listed[:, s : s + 1] == col).astype(F32).astype(BF)
        outs[s][...] = mm(hot, hi) + mm(hot, lo)


def hub_kernel(me, features, hub, *refs, parts):
    outs, full = refs[:parts], refs[parts]
    full[...] = mm(hub[...], features[...].astype(BF))
    size = full.shape[0] // parts
    for s in range(parts):
        at = pl.multiple_of((me[0] ^ s) * size, size)
        outs[s][...] = full[pl.ds(at, size), :]


def inverse_counts(counts):
    return 1.0 / counts[...].astype(F32).T


def count_kernel(features, mine, slots, counts, adj, base, local, *, degree, pool):
    own, _ = features.shape
    rows = mine.shape[0]
    span = GROUP * degree
    near = (own + rows) // LANES
    codes = pool // LANES
    row = lax.broadcasted_iota(jnp.int32, (codes * GROUP, span), 0)
    lane = lax.broadcasted_iota(jnp.int32, (LANES, span), 0)
    vert = lax.broadcasted_iota(jnp.int32, (1, span), 1) // degree

    def build(b, _):
        name = slots[pl.ds(b, 1), :]
        code = jnp.where(name < 0, -1, (name // LANES) * GROUP + vert)
        left = (row == code).astype(F32).astype(BF)
        right = (lane == (name & (LANES - 1))).astype(F32).astype(BF)
        made = mm(left, right, ((1,), (1,))).astype(BF)
        at = pl.multiple_of(b * GROUP, GROUP)
        for h in range(codes):
            part = made[h * GROUP : (h + 1) * GROUP]
            if h < near:
                local[pl.ds(at, GROUP), h * LANES : (h + 1) * LANES] = part
            else:
                adj[pl.ds(at, GROUP), (h - near) * LANES : (h - near + 1) * LANES] = part
        return 0

    lax.fori_loop(0, own // GROUP, build, 0, unroll=4)
    hi, lo = split(jnp.concatenate([features[...], mine[...]], axis=0))
    inv = inverse_counts(counts)
    for j in range(own // LANES):
        cut = slice(j * LANES, (j + 1) * LANES)
        a = local[cut, :]
        base[cut, :] = features[cut, :] + (mm(a, hi) + mm(a, lo)) * inv[:, j : j + 1]


def last_kernel(slot, adj, base, counts, hub, weight, bias, *refs):
    pieces, (out, rhi, rlo, whi, wlo) = refs[:-5], refs[-5:]
    rows, size = base.shape[0], pieces[0].shape[0]
    step = pl.program_id(0)

    @pl.when(step == 0)
    def _():
        for n, piece in enumerate(pieces):
            cut = slice(n * size, (n + 1) * size)
            rhi[cut, :], rlo[cut, :] = split(piece[...])
        whi[...], wlo[...] = split(weight[...])

    inv = inverse_counts(counts)
    a = adj[...]
    summed = mm(a, rhi[...]) + mm(a, rlo[...])
    comb = base[...] + jnp.concatenate(
        [
            summed[j * LANES : (j + 1) * LANES] * inv[:, j : j + 1]
            for j in range(rows // LANES)
        ],
        axis=0,
    )
    row = lax.broadcasted_iota(jnp.int32, (rows, 1), 0) + step * rows
    sums = jnp.sum(hub[...], axis=0)
    for i in range(sums.shape[0]):
        comb = comb + jnp.where(row == slot[i], sums[i : i + 1], 0.0)
    chi, clo = split(comb)
    made = mm(chi, whi[...]) + (mm(chi, wlo[...]) + mm(clo, whi[...])) + bias[...]
    out[...] = jnp.maximum(made, 0.0)


VMEM = pl.BlockSpec(memory_space=pltpu.VMEM)
SMEM = pl.BlockSpec(memory_space=pltpu.SMEM)
PARAMS = pltpu.CompilerParams(vmem_limit_bytes=24 * 1024 * 1024)


def flops(n):
    return pl.CostEstimate(flops=n, bytes_accessed=1 << 20, transcendentals=0)


def on_device(features, hub_block, hub_slot, neighbours, counts, halo_send, weight, bias):
    own, width = features.shape
    degree = neighbours.shape[1]
    n_grp, n_loc = lax.axis_size("grp"), lax.axis_size("loc")
    listed = halo_send.shape[1]
    hubs = hub_block.shape[0]
    owned = hub_slot.shape[0]
    pool = own + n_loc * listed
    here = lax.axis_index("loc").astype(jnp.int32)
    me = jnp.stack([lax.axis_index("grp").astype(jnp.int32), here])

    outgoing = pl.pallas_call(
        functools.partial(pick_kernel, peers=n_loc, rows=listed),
        out_shape=[jax.ShapeDtypeStruct((listed, width), F32)] * n_loc,
        in_specs=[SMEM] + [VMEM] * 2,
        out_specs=[VMEM] * n_loc,
        scratch_shapes=[pltpu.VMEM((n_loc, listed), jnp.int32)],
        compiler_params=PARAMS,
        cost_estimate=flops(4 * n_loc * listed * own * width),
        name="pick",
    )(me, features, halo_send)
    received = []
    for s in range(1, n_loc):
        pairs = [(i, i ^ s) for i in range(n_loc)]
        received.append(lax.ppermute(outgoing[s], "loc", pairs))

    part_rows = hubs // n_grp
    parts = pl.pallas_call(
        functools.partial(hub_kernel, parts=n_grp),
        out_shape=[jax.ShapeDtypeStruct((part_rows, width), F32)] * n_grp,
        in_specs=[SMEM, VMEM, VMEM],
        out_specs=[VMEM] * n_grp,
        scratch_shapes=[pltpu.VMEM((hubs, width), F32)],
        compiler_params=PARAMS,
        cost_estimate=flops(2 * hubs * own * width),
        name="hub",
    )(me, features, hub_block)
    group_part = parts[0]
    for s in range(1, n_grp):
        pairs = [(i, i ^ s) for i in range(n_grp)]
        arrived = lax.ppermute(parts[s], "grp", pairs)
        group_part = group_part + arrived
    group_part = group_part.reshape(n_loc, owned, width)
    hub_pieces = lax.all_to_all(group_part, "loc", split_axis=0, concat_axis=0, tiled=True)

    used = jnp.arange(degree, dtype=jnp.int32)[None, :] < counts[:, None]
    far = neighbours - own
    moved = own + ((far // listed) ^ here) * listed + far % listed
    slots = jnp.where(neighbours < own, neighbours, moved)
    slots = jnp.where(used, slots, -1).reshape(own // GROUP, GROUP * degree)
    counts_rows = counts.reshape(own // LANES, LANES)
    adj, base = pl.pallas_call(
        functools.partial(count_kernel, degree=degree, pool=pool),
        out_shape=[
            jax.ShapeDtypeStruct((own, pool - own - listed), BF),
            jax.ShapeDtypeStruct((own, width), F32),
        ],
        in_specs=[VMEM] * 4,
        out_specs=[VMEM] * 2,
        scratch_shapes=[pltpu.VMEM((own, own + listed), BF)],
        compiler_params=PARAMS,
        cost_estimate=flops(8 * own * own * width),
        name="count",
    )(features, outgoing[0], slots, counts_rows)

    remote = pool - own - listed
    rows = own // STEPS
    whole = lambda *shape: pl.BlockSpec(shape, lambda i: (0,) * len(shape))
    return pl.pallas_call(
        last_kernel,
        out_shape=jax.ShapeDtypeStruct((own, width), F32),
        grid=(STEPS,),
        in_specs=[
            SMEM,
            pl.BlockSpec((rows, remote), lambda i: (i, 0)),
            pl.BlockSpec((rows, width), lambda i: (i, 0)),
            pl.BlockSpec((None, rows // LANES, LANES), lambda i: (i, 0, 0)),
            whole(n_loc, owned, width),
            whole(width, width),
            whole(1, width),
        ]
        + [whole(listed, width)] * (n_loc - 1),
        out_specs=pl.BlockSpec((rows, width), lambda i: (i, 0)),
        scratch_shapes=[pltpu.VMEM((remote, width), BF)] * 2
        + [pltpu.VMEM((width, width), BF)] * 2,
        compiler_params=PARAMS,
        cost_estimate=flops(8 * own * own * width),
        name="last",
    )(
        hub_slot,
        adj,
        base,
        counts.reshape(STEPS, rows // LANES, LANES),
        hub_pieces,
        weight,
        bias.reshape(1, width),
        *received,
    )


def solution(mesh):
    in_specs = (
        P(("grp", "loc"), None),
        P(None, ("grp", "loc")),
        P(("grp", "loc")),
        P(("grp", "loc"), None),
        P(("grp", "loc")),
        P(("grp", "loc"), None),
        P(),
        P(),
    )
    out_specs = P(("grp", "loc"), None)
    return jax.shard_map(
        on_device, mesh=mesh, in_specs=in_specs, out_specs=out_specs, check_vma=False
    )
```

```python
import functools

import jax
import jax.numpy as jnp
from jax import lax
from jax.experimental import pallas as pl
from jax.experimental.pallas import tpu as pltpu
from jax.sharding import PartitionSpec as P


BF = jnp.bfloat16
F32 = jnp.float32
LANES = 128
STEPS = 4
GROUP = 16


def FLOW(peers):
    return sorted(range(1, peers), key=lambda s: (s < 2, s & 1, -s)) + [0]


def split(x):
    hi = x.astype(BF)
    return hi, (x - hi.astype(F32)).astype(BF)


def mm(a, b, dims=((1,), (0,))):
    return lax.dot_general(a, b, (dims, ((), ())), preferred_element_type=F32)


def pick_kernel(me, features, halo, *refs, peers, rows):
    outs, order = refs[:peers], refs[peers]
    hi, lo = split(features[...])
    own = features.shape[0]
    for s in range(peers):
        order[s : s + 1, :] = halo[pl.ds(me[1] ^ s, 1), :]
    listed = order[...].T
    col = lax.broadcasted_iota(jnp.int32, (rows, own), 1)
    for s in FLOW(peers):
        hot = (listed[:, s : s + 1] == col).astype(F32).astype(BF)
        outs[s][...] = mm(hot, hi) + mm(hot, lo)


def hub_kernel(me, features, hub, *refs, parts):
    outs, full = refs[:parts], refs[parts]
    full[...] = mm(hub[...], features[...].astype(BF))
    size = full.shape[0] // parts
    for s in range(parts):
        at = pl.multiple_of((me[0] ^ s) * size, size)
        outs[s][...] = full[pl.ds(at, size), :]


def inverse_counts(counts):
    return 1.0 / counts[...].astype(F32).T


def count_kernel(me, features, mine, names, counts, adj, base, code_s, low_s, near_s, far_s, base_s, sems):
    own, _ = features.shape
    degree = names.shape[0]
    listed = mine.shape[0]
    tiles = own // LANES
    span = GROUP * degree
    each = LANES // GROUP
    near, far = near_s.shape[1] // LANES, far_s.shape[1] // LANES
    codes = near + far

    stacked = jnp.concatenate(
        [names[:, j * LANES : (j + 1) * LANES] for j in range(tiles)], axis=0
    )
    limit = jnp.concatenate(
        [jnp.broadcast_to(counts[j : j + 1, :], (degree, LANES)) for j in range(tiles)], axis=0
    )
    spot = lax.broadcasted_iota(jnp.int32, stacked.shape, 0) % degree
    away = stacked - own
    moved = own + ((away // listed) ^ me[1]) * listed + away % listed
    named = jnp.where(stacked < own, stacked, moved)
    code = jnp.where(spot < limit, named // LANES, -1).astype(F32).astype(BF)
    low = (named % LANES).astype(F32).astype(BF)
    wide = (LANES, each * span)
    lane = lax.broadcasted_iota(jnp.int32, wide, 1)
    vertex = lax.broadcasted_iota(jnp.int32, wide, 0)
    choose = (vertex == (lane // span) * GROUP + lane % GROUP).astype(F32).astype(BF)
    rows = (tiles * degree, each * span)
    lane = lax.broadcasted_iota(jnp.int32, rows, 1)
    kept = lax.broadcasted_iota(jnp.int32, rows, 0) % degree == (lane % span) // GROUP

    def line_up(x):
        spread = jnp.where(kept, mm(x, choose), 0.0)
        return jnp.sum(spread.reshape(tiles, degree, each * span), axis=1)

    member = (lax.broadcasted_iota(jnp.int32, (1, each * span), 1) % GROUP).astype(F32)
    code_s[...] = line_up(code) * GROUP + member
    low_s[...] = line_up(low)

    kind = BF if codes * GROUP <= 256 else F32
    row = lax.broadcasted_iota(jnp.int32, (codes * GROUP, span), 0).astype(F32).astype(kind)
    bits = lax.broadcasted_iota(jnp.int32, (LANES, span), 0).astype(F32).astype(BF)

    def hot(x, y):
        return jnp.where(x == y, jnp.ones((), x.dtype), jnp.zeros((), x.dtype)).astype(BF)

    def build(j, _):
        for e in range(each):
            cut = slice(e * span, (e + 1) * span)
            left = hot(row, code_s[pl.ds(j, 1), cut].astype(kind))
            right = hot(bits, low_s[pl.ds(j, 1), cut].astype(BF))
            made = mm(left, right, ((1,), (1,))).astype(BF)
            at = pl.multiple_of(j * LANES + e * GROUP, GROUP)
            for h in range(codes):
                part = made[h * GROUP : (h + 1) * GROUP]
                to, k = (near_s, h) if h < near else (far_s, h - near)
                to[pl.ds(at, GROUP), k * LANES : (k + 1) * LANES] = part
        return 0

    lax.fori_loop(0, tiles, build, 0)
    first = pltpu.make_async_copy(far_s, adj, sems.at[0])
    first.start()
    hi, lo = split(jnp.concatenate([features[...], mine[...]], axis=0))
    inv = inverse_counts(counts)
    for j in range(tiles):
        cut = slice(j * LANES, (j + 1) * LANES)
        a = near_s[cut, :]
        base_s[cut, :] = features[cut, :] + (mm(a, hi) + mm(a, lo)) * inv[:, j : j + 1]
    second = pltpu.make_async_copy(base_s, base, sems.at[1])
    second.start()
    first.wait()
    second.wait()


def last_kernel(slot, adj, base, counts, hub, weight, bias, *refs):
    pieces, (out, adj_s, base_s, out_s, rhi, rlo, ins, ends) = refs[:-8], refs[-8:]
    size = pieces[0].shape[0]
    rows = adj_s.shape[0] // STEPS
    cuts = [pl.ds(n * rows, rows) for n in range(STEPS)]
    loads = []
    for n, cut in enumerate(cuts):
        loads.append(pltpu.make_async_copy(adj.at[cut], adj_s.at[cut], ins.at[2 * n]))
        loads.append(pltpu.make_async_copy(base.at[cut], base_s.at[cut], ins.at[2 * n + 1]))
    for load in loads:
        load.start()
    for n, piece in enumerate(pieces):
        cut = slice(n * size, (n + 1) * size)
        rhi[cut, :], rlo[cut, :] = split(piece[...])
    whi, wlo = split(weight[...])
    inv = inverse_counts(counts)
    sums = jnp.sum(hub[...], axis=0)
    per = rows // LANES
    stores = []
    for n, cut in enumerate(cuts):
        loads[2 * n].wait()
        loads[2 * n + 1].wait()
        a = adj_s[cut, :]
        summed = mm(a, rhi[...]) + mm(a, rlo[...])
        scale = jnp.concatenate([inv[:, n * per + j : n * per + j + 1] for j in range(per)], axis=0)
        comb = base_s[cut, :] + summed * scale
        row = lax.broadcasted_iota(jnp.int32, (rows, 1), 0) + n * rows
        for i in range(sums.shape[0]):
            comb = comb + jnp.where(row == slot[i], sums[i : i + 1], 0.0)
        chi, clo = split(comb)
        made = mm(chi, whi) + (mm(chi, wlo) + mm(clo, whi)) + bias[...]
        out_s[cut, :] = jnp.maximum(made, 0.0)
        store = pltpu.make_async_copy(out_s.at[cut], out.at[cut], ends.at[n])
        store.start()
        stores.append(store)
    for store in stores:
        store.wait()


VMEM = pl.BlockSpec(memory_space=pltpu.VMEM)
HBM = pl.BlockSpec(memory_space=pltpu.HBM)
SMEM = pl.BlockSpec(memory_space=pltpu.SMEM)
PARAMS = pltpu.CompilerParams(vmem_limit_bytes=24 * 1024 * 1024)


def flops(n):
    return pl.CostEstimate(flops=n, bytes_accessed=1 << 20, transcendentals=0)


def on_device(features, hub_block, hub_slot, neighbours, counts, halo_send, weight, bias):
    own, width = features.shape
    degree = neighbours.shape[1]
    n_grp, n_loc = lax.axis_size("grp"), lax.axis_size("loc")
    listed = halo_send.shape[1]
    hubs = hub_block.shape[0]
    owned = hub_slot.shape[0]
    pool = own + n_loc * listed
    here = lax.axis_index("loc").astype(jnp.int32)
    me = jnp.stack([lax.axis_index("grp").astype(jnp.int32), here])

    outgoing = pl.pallas_call(
        functools.partial(pick_kernel, peers=n_loc, rows=listed),
        out_shape=[jax.ShapeDtypeStruct((listed, width), F32)] * n_loc,
        in_specs=[SMEM] + [VMEM] * 2,
        out_specs=[VMEM] * n_loc,
        scratch_shapes=[pltpu.VMEM((n_loc, listed), jnp.int32)],
        compiler_params=PARAMS,
        cost_estimate=flops(4 * n_loc * listed * own * width),
        name="pick",
    )(me, features, halo_send)
    received = []
    for s in range(1, n_loc):
        pairs = [(i, i ^ s) for i in range(n_loc)]
        received.append(lax.ppermute(outgoing[s], "loc", pairs))

    part_rows = hubs // n_grp
    parts = pl.pallas_call(
        functools.partial(hub_kernel, parts=n_grp),
        out_shape=[jax.ShapeDtypeStruct((part_rows, width), F32)] * n_grp,
        in_specs=[SMEM, VMEM, VMEM],
        out_specs=[VMEM] * n_grp,
        scratch_shapes=[pltpu.VMEM((hubs, width), F32)],
        compiler_params=PARAMS,
        cost_estimate=flops(2 * hubs * own * width),
        name="hub",
    )(me, features, hub_block)
    group_part = parts[0]
    for s in range(1, n_grp):
        pairs = [(i, i ^ s) for i in range(n_grp)]
        arrived = lax.ppermute(parts[s], "grp", pairs)
        group_part = group_part + arrived
    group_part = group_part.reshape(n_loc, owned, width)
    hub_pieces = lax.all_to_all(group_part, "loc", split_axis=0, concat_axis=0, tiled=True)

    remote = pool - own - listed
    tiles = own // LANES
    counts_rows = counts.reshape(tiles, LANES)
    line = (tiles, LANES * degree)
    adj, base = pl.pallas_call(
        count_kernel,
        out_shape=[
            pltpu.HBM((own, remote), BF),
            pltpu.HBM((own, width), F32),
        ],
        in_specs=[SMEM] + [VMEM] * 4,
        out_specs=[HBM] * 2,
        scratch_shapes=[
            pltpu.VMEM(line, F32),
            pltpu.VMEM(line, F32),
            pltpu.VMEM((own, own + listed), BF),
            pltpu.VMEM((own, remote), BF),
            pltpu.VMEM((own, width), F32),
            pltpu.SemaphoreType.DMA((2,)),
        ],
        compiler_params=PARAMS,
        cost_estimate=flops(8 * own * own * width),
        name="count",
    )(me, features, outgoing[0], neighbours.T, counts_rows)

    adj = pltpu.with_memory_space_constraint(adj, pltpu.HBM)
    base = pltpu.with_memory_space_constraint(base, pltpu.HBM)
    return pl.pallas_call(
        last_kernel,
        out_shape=jax.ShapeDtypeStruct((own, width), F32),
        in_specs=[SMEM, HBM, HBM] + [VMEM] * (4 + len(received)),
        out_specs=HBM,
        scratch_shapes=[
            pltpu.VMEM((own, remote), BF),
            pltpu.VMEM((own, width), F32),
            pltpu.VMEM((own, width), F32),
            pltpu.VMEM((remote, width), BF),
            pltpu.VMEM((remote, width), BF),
            pltpu.SemaphoreType.DMA((2 * STEPS,)),
            pltpu.SemaphoreType.DMA((STEPS,)),
        ],
        compiler_params=PARAMS,
        cost_estimate=flops(8 * own * own * width),
        name="last",
    )(
        hub_slot, adj, base, counts_rows, hub_pieces, weight, bias.reshape(1, width), *received
    )


def solution(mesh):
    in_specs = (
        P(("grp", "loc"), None),
        P(None, ("grp", "loc")),
        P(("grp", "loc")),
        P(("grp", "loc"), None),
        P(("grp", "loc")),
        P(("grp", "loc"), None),
        P(),
        P(),
    )
    out_specs = P(("grp", "loc"), None)
    return jax.shard_map(
        on_device, mesh=mesh, in_specs=in_specs, out_specs=out_specs, check_vma=False
    )
```

```python
import functools

import jax
import jax.numpy as jnp
from jax import lax
from jax.experimental import pallas as pl
from jax.experimental.pallas import tpu as pltpu
from jax.sharding import PartitionSpec as P


BF = jnp.bfloat16
F32 = jnp.float32
LANES = 128
STEPS = 4
GROUP = 16


def FLOW(peers):
    return sorted(range(1, peers), key=lambda s: (s < 2, s & 1, -s)) + [0]


def split(x):
    hi = x.astype(BF)
    return hi, (x - hi.astype(F32)).astype(BF)


def mm(a, b, dims=((1,), (0,))):
    return lax.dot_general(a, b, (dims, ((), ())), preferred_element_type=F32)


def pick_kernel(me, features, halo, *refs, peers, rows):
    outs, order = refs[:peers], refs[peers]
    hi, lo = split(features[...])
    own = features.shape[0]
    for s in range(peers):
        order[s : s + 1, :] = halo[pl.ds(me[1] ^ s, 1), :]
    listed = order[...].T
    col = lax.broadcasted_iota(jnp.int32, (rows, own), 1)
    for s in FLOW(peers):
        hot = (listed[:, s : s + 1] == col).astype(F32).astype(BF)
        outs[s][...] = mm(hot, hi) + mm(hot, lo)


def hub_kernel(me, features, hub, *refs, parts):
    outs, full = refs[:parts], refs[parts]
    full[...] = mm(hub[...], features[...].astype(BF))
    size = full.shape[0] // parts
    for s in range(parts):
        at = pl.multiple_of((me[0] ^ s) * size, size)
        outs[s][...] = full[pl.ds(at, size), :]


def fold_kernel(me, *refs, parts, peers):
    ins, outs, full = refs[:parts], refs[parts:-1], refs[-1]
    total = ins[0][...]
    for piece in ins[1:]:
        total = total + piece[...]
    full[...] = total
    size = full.shape[0] // peers
    for s in range(peers):
        for i in range(size):
            outs[s][i : i + 1, :] = full[pl.ds((me[1] ^ s) * size + i, 1), :]


def inverse_counts(counts):
    return 1.0 / counts[...].astype(F32).T


def count_kernel(me, features, mine, names, counts, far_s, base, code_s, low_s, near_s):
    own, _ = features.shape
    degree = names.shape[0]
    listed = mine.shape[0]
    tiles = own // LANES
    span = GROUP * degree
    each = LANES // GROUP
    near, far = near_s.shape[1] // LANES, far_s.shape[1] // LANES
    codes = near + far

    stacked = jnp.concatenate(
        [names[:, j * LANES : (j + 1) * LANES] for j in range(tiles)], axis=0
    )
    limit = jnp.concatenate(
        [jnp.broadcast_to(counts[j : j + 1, :], (degree, LANES)) for j in range(tiles)], axis=0
    )
    spot = lax.broadcasted_iota(jnp.int32, stacked.shape, 0) % degree
    away = stacked - own
    moved = own + ((away // listed) ^ me[1]) * listed + away % listed
    named = jnp.where(stacked < own, stacked, moved)
    code = jnp.where(spot < limit, named // LANES, -1).astype(F32).astype(BF)
    low = (named % LANES).astype(F32).astype(BF)
    wide = (LANES, each * span)
    lane = lax.broadcasted_iota(jnp.int32, wide, 1)
    vertex = lax.broadcasted_iota(jnp.int32, wide, 0)
    choose = (vertex == (lane // span) * GROUP + lane % GROUP).astype(F32).astype(BF)
    rows = (tiles * degree, each * span)
    lane = lax.broadcasted_iota(jnp.int32, rows, 1)
    kept = lax.broadcasted_iota(jnp.int32, rows, 0) % degree == (lane % span) // GROUP

    def line_up(x):
        spread = jnp.where(kept, mm(x, choose), 0.0)
        return jnp.sum(spread.reshape(tiles, degree, each * span), axis=1)

    member = (lax.broadcasted_iota(jnp.int32, (1, each * span), 1) % GROUP).astype(F32)
    code_s[...] = line_up(code) * GROUP + member
    low_s[...] = line_up(low)

    kind = BF if codes * GROUP <= 256 else F32
    row = lax.broadcasted_iota(jnp.int32, (codes * GROUP, span), 0).astype(F32).astype(kind)
    bits = lax.broadcasted_iota(jnp.int32, (LANES, span), 0).astype(F32).astype(BF)

    def hot(x, y):
        return jnp.where(x == y, jnp.ones((), x.dtype), jnp.zeros((), x.dtype)).astype(BF)

    def build(j, _):
        for e in range(each):
            cut = slice(e * span, (e + 1) * span)
            left = hot(row, code_s[pl.ds(j, 1), cut].astype(kind))
            right = hot(bits, low_s[pl.ds(j, 1), cut].astype(BF))
            made = mm(left, right, ((1,), (1,))).astype(BF)
            at = pl.multiple_of(j * LANES + e * GROUP, GROUP)
            for h in range(codes):
                part = made[h * GROUP : (h + 1) * GROUP]
                to, k = (near_s, h) if h < near else (far_s, h - near)
                to[pl.ds(at, GROUP), k * LANES : (k + 1) * LANES] = part
        return 0

    lax.fori_loop(0, tiles, build, 0)
    hi, lo = split(jnp.concatenate([features[...], mine[...]], axis=0))
    inv = inverse_counts(counts)
    for j in range(tiles):
        cut = slice(j * LANES, (j + 1) * LANES)
        a = near_s[cut, :]
        base[cut, :] = features[cut, :] + (mm(a, hi) + mm(a, lo)) * inv[:, j : j + 1]


def last_kernel(slot, adj, base, counts, weight, bias, *refs, peers):
    hubs, pieces, (out, out_s, rhi, rlo, ends) = refs[:peers], refs[peers:-5], refs[-5:]
    size = pieces[0].shape[0]
    rows = adj.shape[0] // STEPS
    cuts = [pl.ds(n * rows, rows) for n in range(STEPS)]
    for n, piece in enumerate(pieces):
        cut = slice(n * size, (n + 1) * size)
        rhi[cut, :], rlo[cut, :] = split(piece[...])
    whi, wlo = split(weight[...])
    inv = inverse_counts(counts)
    sums = hubs[0][...]
    for hub in hubs[1:]:
        sums = sums + hub[...]
    per = rows // LANES
    stores = []
    for n, cut in enumerate(cuts):
        a = adj[cut, :]
        summed = mm(a, rhi[...]) + mm(a, rlo[...])
        scale = jnp.concatenate([inv[:, n * per + j : n * per + j + 1] for j in range(per)], axis=0)
        comb = base[cut, :] + summed * scale
        row = lax.broadcasted_iota(jnp.int32, (rows, 1), 0) + n * rows
        for i in range(sums.shape[0]):
            comb = comb + jnp.where(row == slot[i], sums[i : i + 1], 0.0)
        chi, clo = split(comb)
        made = mm(chi, whi) + (mm(chi, wlo) + mm(clo, whi)) + bias[...]
        out_s[cut, :] = jnp.maximum(made, 0.0)
        store = pltpu.make_async_copy(out_s.at[cut], out.at[cut], ends.at[n])
        store.start()
        stores.append(store)
    for store in stores:
        store.wait()


VMEM = pl.BlockSpec(memory_space=pltpu.VMEM)
HBM = pl.BlockSpec(memory_space=pltpu.HBM)
SMEM = pl.BlockSpec(memory_space=pltpu.SMEM)
PARAMS = pltpu.CompilerParams(vmem_limit_bytes=24 * 1024 * 1024)


def flops(n):
    return pl.CostEstimate(flops=n, bytes_accessed=1 << 20, transcendentals=0)


def on_device(features, hub_block, hub_slot, neighbours, counts, halo_send, weight, bias):
    own, width = features.shape
    degree = neighbours.shape[1]
    n_grp, n_loc = lax.axis_size("grp"), lax.axis_size("loc")
    listed = halo_send.shape[1]
    hubs = hub_block.shape[0]
    owned = hub_slot.shape[0]
    pool = own + n_loc * listed
    here = lax.axis_index("loc").astype(jnp.int32)
    me = jnp.stack([lax.axis_index("grp").astype(jnp.int32), here])

    outgoing = pl.pallas_call(
        functools.partial(pick_kernel, peers=n_loc, rows=listed),
        out_shape=[jax.ShapeDtypeStruct((listed, width), F32)] * n_loc,
        in_specs=[SMEM] + [VMEM] * 2,
        out_specs=[VMEM] * n_loc,
        scratch_shapes=[pltpu.VMEM((n_loc, listed), jnp.int32)],
        compiler_params=PARAMS,
        cost_estimate=flops(4 * n_loc * listed * own * width),
        name="pick",
    )(me, features, halo_send)
    received = []
    for s in range(1, n_loc):
        pairs = [(i, i ^ s) for i in range(n_loc)]
        received.append(lax.ppermute(outgoing[s], "loc", pairs))

    part_rows = hubs // n_grp
    parts = pl.pallas_call(
        functools.partial(hub_kernel, parts=n_grp),
        out_shape=[jax.ShapeDtypeStruct((part_rows, width), F32)] * n_grp,
        in_specs=[SMEM, VMEM, VMEM],
        out_specs=[VMEM] * n_grp,
        scratch_shapes=[pltpu.VMEM((hubs, width), F32)],
        compiler_params=PARAMS,
        cost_estimate=flops(2 * hubs * own * width),
        name="hub",
    )(me, features, hub_block)
    arrived = [parts[0]]
    for s in range(1, n_grp):
        pairs = [(i, i ^ s) for i in range(n_grp)]
        arrived.append(lax.ppermute(parts[s], "grp", pairs))
    folded = pl.pallas_call(
        functools.partial(fold_kernel, parts=n_grp, peers=n_loc),
        out_shape=[jax.ShapeDtypeStruct((owned, width), F32)] * n_loc,
        in_specs=[SMEM] + [VMEM] * n_grp,
        out_specs=[VMEM] * n_loc,
        scratch_shapes=[pltpu.VMEM((part_rows, width), F32)],
        compiler_params=PARAMS,
        name="fold",
    )(me, *arrived)
    hub_pieces = [folded[0]]
    for s in range(1, n_loc):
        pairs = [(i, i ^ s) for i in range(n_loc)]
        hub_pieces.append(lax.ppermute(folded[s], "loc", pairs))

    remote = pool - own - listed
    tiles = own // LANES
    counts_rows = counts.reshape(tiles, LANES)
    line = (tiles, LANES * degree)
    adj, base = pl.pallas_call(
        count_kernel,
        out_shape=[
            jax.ShapeDtypeStruct((own, remote), BF),
            jax.ShapeDtypeStruct((own, width), F32),
        ],
        in_specs=[SMEM] + [VMEM] * 4,
        out_specs=[VMEM] * 2,
        scratch_shapes=[
            pltpu.VMEM(line, F32),
            pltpu.VMEM(line, F32),
            pltpu.VMEM((own, own + listed), BF),
        ],
        compiler_params=PARAMS,
        cost_estimate=flops(8 * own * own * width),
        name="count",
    )(me, features, outgoing[0], neighbours.T, counts_rows)

    return pl.pallas_call(
        functools.partial(last_kernel, peers=n_loc),
        out_shape=jax.ShapeDtypeStruct((own, width), F32),
        in_specs=[SMEM] + [VMEM] * (5 + len(hub_pieces) + len(received)),
        out_specs=HBM,
        scratch_shapes=[
            pltpu.VMEM((own, width), F32),
            pltpu.VMEM((remote, width), BF),
            pltpu.VMEM((remote, width), BF),
            pltpu.SemaphoreType.DMA((STEPS,)),
        ],
        compiler_params=PARAMS,
        cost_estimate=flops(8 * own * own * width),
        name="last",
    )(
        hub_slot, adj, base, counts_rows, weight, bias.reshape(1, width), *hub_pieces, *received
    )


def solution(mesh):
    in_specs = (
        P(("grp", "loc"), None),
        P(None, ("grp", "loc")),
        P(("grp", "loc")),
        P(("grp", "loc"), None),
        P(("grp", "loc")),
        P(("grp", "loc"), None),
        P(),
        P(),
    )
    out_specs = P(("grp", "loc"), None)
    return jax.shard_map(
        on_device, mesh=mesh, in_specs=in_specs, out_specs=out_specs, check_vma=False
    )
```

```python
import functools

import jax
import jax.numpy as jnp
from jax import lax
from jax.experimental import pallas as pl
from jax.experimental.pallas import tpu as pltpu
from jax.sharding import PartitionSpec as P


BF = jnp.bfloat16
F32 = jnp.float32
LANES = 128
GROUP = 16


def FLOW(peers):
    return sorted(range(1, peers), key=lambda s: (s < 2, s & 1, -s)) + [0]


def split(x):
    hi = x.astype(BF)
    return hi, (x - hi.astype(F32)).astype(BF)


def mm(a, b, dims=((1,), (0,))):
    return lax.dot_general(a, b, (dims, ((), ())), preferred_element_type=F32)


def pick_kernel(me, features, halo, *refs, peers, rows):
    outs, order = refs[:peers], refs[peers]
    hi, lo = split(features[...])
    own = features.shape[0]
    for s in range(peers):
        order[s : s + 1, :] = halo[pl.ds(me[1] ^ s, 1), :]
    listed = order[...].T
    col = lax.broadcasted_iota(jnp.int32, (rows, own), 1)
    for s in FLOW(peers):
        hot = (listed[:, s : s + 1] == col).astype(F32).astype(BF)
        outs[s][...] = mm(hot, hi) + mm(hot, lo)


def hub_kernel(me, features, hub, *refs, parts):
    outs, full = refs[:parts], refs[parts]
    full[...] = mm(hub[...], features[...].astype(BF))
    size = full.shape[0] // parts
    for s in range(parts):
        at = pl.multiple_of((me[0] ^ s) * size, size)
        outs[s][...] = full[pl.ds(at, size), :]


def fold_kernel(me, *refs, parts, peers):
    ins, outs, full = refs[:parts], refs[parts:-1], refs[-1]
    total = ins[0][...]
    for piece in ins[1:]:
        total = total + piece[...]
    full[...] = total
    size = full.shape[0] // peers
    for s in range(peers):
        for i in range(size):
            outs[s][i : i + 1, :] = full[pl.ds((me[1] ^ s) * size + i, 1), :]


def inverse_counts(counts):
    return 1.0 / counts[...].astype(F32).T


def count_kernel(me, names, counts, near_s, far_s, code_s, low_s, *, listed):
    degree, own = names.shape
    tiles = own // LANES
    span = GROUP * degree
    each = LANES // GROUP
    near, far = near_s.shape[1] // LANES, far_s.shape[1] // LANES
    codes = near + far

    stacked = jnp.concatenate(
        [names[:, j * LANES : (j + 1) * LANES] for j in range(tiles)], axis=0
    )
    limit = jnp.concatenate(
        [jnp.broadcast_to(counts[j : j + 1, :], (degree, LANES)) for j in range(tiles)], axis=0
    )
    spot = lax.broadcasted_iota(jnp.int32, stacked.shape, 0) % degree
    away = stacked - own
    moved = own + ((away // listed) ^ me[1]) * listed + away % listed
    named = jnp.where(stacked < own, stacked, moved)
    code = jnp.where(spot < limit, named // LANES, -1).astype(F32).astype(BF)
    low = (named % LANES).astype(F32).astype(BF)
    wide = (LANES, each * span)
    lane = lax.broadcasted_iota(jnp.int32, wide, 1)
    vertex = lax.broadcasted_iota(jnp.int32, wide, 0)
    choose = (vertex == (lane // span) * GROUP + lane % GROUP).astype(F32).astype(BF)
    rows = (tiles * degree, each * span)
    lane = lax.broadcasted_iota(jnp.int32, rows, 1)
    kept = lax.broadcasted_iota(jnp.int32, rows, 0) % degree == (lane % span) // GROUP

    def line_up(x):
        spread = jnp.where(kept, mm(x, choose), 0.0)
        return jnp.sum(spread.reshape(tiles, degree, each * span), axis=1)

    member = (lax.broadcasted_iota(jnp.int32, (1, each * span), 1) % GROUP).astype(F32)
    code_s[...] = line_up(code) * GROUP + member
    low_s[...] = line_up(low)

    kind = BF if codes * GROUP <= 256 else F32
    row = lax.broadcasted_iota(jnp.int32, (codes * GROUP, span), 0).astype(F32).astype(kind)
    bits = lax.broadcasted_iota(jnp.int32, (LANES, span), 0).astype(F32).astype(BF)

    def hot(x, y):
        return jnp.where(x == y, jnp.ones((), x.dtype), jnp.zeros((), x.dtype)).astype(BF)

    def build(j, _):
        for e in range(each):
            cut = slice(e * span, (e + 1) * span)
            left = hot(row, code_s[pl.ds(j, 1), cut].astype(kind))
            right = hot(bits, low_s[pl.ds(j, 1), cut].astype(BF))
            made = mm(left, right, ((1,), (1,))).astype(BF)
            at = pl.multiple_of(j * LANES + e * GROUP, GROUP)
            for h in range(codes):
                part = made[h * GROUP : (h + 1) * GROUP]
                to, k = (near_s, h) if h < near else (far_s, h - near)
                to[pl.ds(at, GROUP), k * LANES : (k + 1) * LANES] = part
        return 0

    lax.fori_loop(0, tiles, build, 0)


def near_kernel(near, features, mine, counts, base):
    hi, lo = split(jnp.concatenate([features[...], mine[...]], axis=0))
    inv = inverse_counts(counts)
    for j in range(near.shape[0] // LANES):
        cut = slice(j * LANES, (j + 1) * LANES)
        a = near[cut, :]
        base[cut, :] = features[cut, :] + (mm(a, hi) + mm(a, lo)) * inv[:, j : j + 1]


def last_kernel(slot, adj, base, counts, weight, bias, *refs, peers):
    hubs, pieces, (out, comb, out_s, ends) = refs[:peers], refs[peers:-4], refs[-4:]
    hi, lo = split(jnp.concatenate([piece[...] for piece in pieces], axis=0))
    inv = inverse_counts(counts)
    cuts = [slice(j * LANES, (j + 1) * LANES) for j in range(adj.shape[0] // LANES)]
    for j, cut in enumerate(cuts):
        a = adj[cut, :]
        comb[cut, :] = base[cut, :] + (mm(a, hi) + mm(a, lo)) * inv[:, j : j + 1]
    sums = hubs[0][...]
    for hub in hubs[1:]:
        sums = sums + hub[...]
    for i in range(sums.shape[0]):
        at = slot[i]
        comb[pl.ds(at, 1), :] = comb[pl.ds(at, 1), :] + sums[i : i + 1]
    whi, wlo = split(weight[...])
    stores = []
    for j, cut in enumerate(cuts):
        chi, clo = split(comb[cut, :])
        made = mm(chi, whi) + (mm(chi, wlo) + mm(clo, whi)) + bias[...]
        out_s[cut, :] = jnp.maximum(made, 0.0)
        store = pltpu.make_async_copy(out_s.at[cut], out.at[cut], ends.at[j])
        store.start()
        stores.append(store)
    for store in stores:
        store.wait()


VMEM = pl.BlockSpec(memory_space=pltpu.VMEM)
HBM = pl.BlockSpec(memory_space=pltpu.HBM)
SMEM = pl.BlockSpec(memory_space=pltpu.SMEM)
PARAMS = pltpu.CompilerParams(vmem_limit_bytes=24 * 1024 * 1024)


def flops(n):
    return pl.CostEstimate(flops=n, bytes_accessed=1 << 20, transcendentals=0)


def on_device(features, hub_block, hub_slot, neighbours, counts, halo_send, weight, bias):
    own, width = features.shape
    degree = neighbours.shape[1]
    n_grp, n_loc = lax.axis_size("grp"), lax.axis_size("loc")
    listed = halo_send.shape[1]
    hubs = hub_block.shape[0]
    owned = hub_slot.shape[0]
    pool = own + n_loc * listed
    here = lax.axis_index("loc").astype(jnp.int32)
    me = jnp.stack([lax.axis_index("grp").astype(jnp.int32), here])

    outgoing = pl.pallas_call(
        functools.partial(pick_kernel, peers=n_loc, rows=listed),
        out_shape=[jax.ShapeDtypeStruct((listed, width), F32)] * n_loc,
        in_specs=[SMEM] + [VMEM] * 2,
        out_specs=[VMEM] * n_loc,
        scratch_shapes=[pltpu.VMEM((n_loc, listed), jnp.int32)],
        compiler_params=PARAMS,
        cost_estimate=flops(4 * n_loc * listed * own * width),
        name="pick",
    )(me, features, halo_send)
    received = []
    for s in range(1, n_loc):
        pairs = [(i, i ^ s) for i in range(n_loc)]
        received.append(lax.ppermute(outgoing[s], "loc", pairs))

    part_rows = hubs // n_grp
    parts = pl.pallas_call(
        functools.partial(hub_kernel, parts=n_grp),
        out_shape=[jax.ShapeDtypeStruct((part_rows, width), F32)] * n_grp,
        in_specs=[SMEM, VMEM, VMEM],
        out_specs=[VMEM] * n_grp,
        scratch_shapes=[pltpu.VMEM((hubs, width), F32)],
        compiler_params=PARAMS,
        cost_estimate=flops(2 * hubs * own * width),
        name="hub",
    )(me, features, hub_block)
    arrived = [parts[0]]
    for s in range(1, n_grp):
        pairs = [(i, i ^ s) for i in range(n_grp)]
        arrived.append(lax.ppermute(parts[s], "grp", pairs))
    folded = pl.pallas_call(
        functools.partial(fold_kernel, parts=n_grp, peers=n_loc),
        out_shape=[jax.ShapeDtypeStruct((owned, width), F32)] * n_loc,
        in_specs=[SMEM] + [VMEM] * n_grp,
        out_specs=[VMEM] * n_loc,
        scratch_shapes=[pltpu.VMEM((part_rows, width), F32)],
        compiler_params=PARAMS,
        name="fold",
    )(me, *arrived)
    hub_pieces = [folded[0]]
    for s in range(1, n_loc):
        pairs = [(i, i ^ s) for i in range(n_loc)]
        hub_pieces.append(lax.ppermute(folded[s], "loc", pairs))

    remote = pool - own - listed
    tiles = own // LANES
    counts_rows = counts.reshape(tiles, LANES)
    line = (tiles, LANES * degree)
    near, adj = pl.pallas_call(
        functools.partial(count_kernel, listed=listed),
        out_shape=[
            jax.ShapeDtypeStruct((own, own + listed), BF),
            jax.ShapeDtypeStruct((own, remote), BF),
        ],
        in_specs=[SMEM] + [VMEM] * 2,
        out_specs=[VMEM] * 2,
        scratch_shapes=[pltpu.VMEM(line, F32)] * 2,
        compiler_params=PARAMS,
        cost_estimate=flops(4 * own * own * width),
        name="count",
    )(me, neighbours.T, counts_rows)
    base = pl.pallas_call(
        near_kernel,
        out_shape=jax.ShapeDtypeStruct((own, width), F32),
        in_specs=[VMEM] * 4,
        out_specs=VMEM,
        compiler_params=PARAMS,
        cost_estimate=flops(4 * own * own * width),
        name="near",
    )(near, features, outgoing[0], counts_rows)

    return pl.pallas_call(
        functools.partial(last_kernel, peers=n_loc),
        out_shape=jax.ShapeDtypeStruct((own, width), F32),
        in_specs=[SMEM] + [VMEM] * (5 + len(hub_pieces) + len(received)),
        out_specs=HBM,
        scratch_shapes=[
            pltpu.VMEM((own, width), F32),
            pltpu.VMEM((own, width), F32),
            pltpu.SemaphoreType.DMA((tiles,)),
        ],
        compiler_params=PARAMS,
        cost_estimate=flops(8 * own * own * width),
        name="last",
    )(
        hub_slot, adj, base, counts_rows, weight, bias.reshape(1, width), *hub_pieces, *received
    )


def solution(mesh):
    in_specs = (
        P(("grp", "loc"), None),
        P(None, ("grp", "loc")),
        P(("grp", "loc")),
        P(("grp", "loc"), None),
        P(("grp", "loc")),
        P(("grp", "loc"), None),
        P(),
        P(),
    )
    out_specs = P(("grp", "loc"), None)
    return jax.shard_map(
        on_device, mesh=mesh, in_specs=in_specs, out_specs=out_specs, check_vma=False
    )
```
